32 devices in a mesh: seq: 16 (over z, y, x), head: 2 (over core).
Axes of the slice: x: 2, y: 2, z: 4, core: 2. Of those that a mesh axis runs over, the one named last changes fastest.
Arguments:
- hidden: bfloat16 [8192, 8192], P('seq', 'head'), may hold values from -6 to 6
- key_weight: bfloat16 [8192, 1024], P('head'), may hold values from -0.0625 to 0.0625
- value_weight: bfloat16 [8192, 1024], P('head'), may hold values from -0.0625 to 0.0625
- key_bias: float32 [1024], P('head'), may hold values from -5 to 5
- value_bias: float32 [1024], P('head'), may hold values from -5 to 5
- request_tokens: int32 [16], replicated, may hold values from 1 to 1024, 8192 in all
- request_context: int32 [16], replicated, may hold values from 0 to 4095
- page_owner: int32 [1024], replicated, may hold values from 0 to 15, as said below
- page_slot: int32 [1024], replicated, may hold values from 0 to 78
- key_cache: bfloat16 [1264, 8, 1024], P('seq', None, 'head'), may hold values from -1 to 1
- value_cache: bfloat16 [1264, 8, 1024], P('seq', None, 'head'), may hold values from -1 to 1
- stored_key_scales: bfloat16 [1264, 8], P('seq', 'head'), may hold values from 0.5 to 8
- value_scales: bfloat16 [1264, 8], P('seq', 'head'), may hold values from 0.5 to 8
Outputs:
- new_key_cache: bfloat16 [1264, 8, 1024], P('seq', None, 'head')
- new_value_cache: bfloat16 [1264, 8, 1024], P('seq', None, 'head')
- new_key_scales: bfloat16 [1264, 8], P('seq', 'head')
- new_value_scales: bfloat16 [1264, 8], P('seq', 'head')
The draws below stay inside these ranges and needn't reach their ends.
Inputs may be any that keep to these rules, and one draw needn't show every extreme that they name: No two pages name the same (page_owner, page_slot) pair. Each index of seq owns at most 79 pages of the block, and one owns exactly 79 in every draw. The 64 pages of one index of seq (pages i * 64 to (i + 1) * 64 - 1) go at most 5 to one owner, and some index sends exactly 5 to one owner in every draw.
All inputs are finite; a program needn't handle non-finite values.
Results may differ from the reference program's by a relative error of at most 0.0065.
Values may be sent and summed in bfloat16 or wider, within the bound.
A program may use at most 128 MiB of HBM per device.

```python
import math
import jax
import jax.numpy as jnp
import numpy as np

D = 8192
KVH = 8
HD = 128
PAGE = 8
REQS = 16
TOKENS = 8192
PAGES_DEV = 64
PAGES = 1024
SLOTS_DEV = 79
SLOTS = 1264
N_SEQ = 16


def page_table(key):
    base_key = jax.random.fold_in(key, 7)
    first, second, third, fourth = jax.random.split(base_key, 4)
    count = N_SEQ
    per_dev = PAGES_DEV
    window = SLOTS_DEV - PAGES_DEV
    order = jax.random.permutation(first, count)
    shift_zero = jax.random.randint(second, (), 0, count)
    hot_index = jax.random.randint(third, (), 0, count)
    page_ids = jnp.arange(count * per_dev).astype(jnp.int32)
    senders = page_ids // per_dev
    within = page_ids % per_dev
    normal_index = (senders + shift_zero - within) % count
    anchor = (hot_index - shift_zero) % count
    distance = (senders - anchor) % count
    moved = (within == 0) & (distance >= 1) & (distance <= window)
    index = jnp.where(moved, hot_index, normal_index)
    owner = order[index].astype(jnp.int32)
    earlier = (owner[:, None] == owner[None, :]) & (page_ids[None, :] < page_ids[:, None])
    rank = jnp.sum(earlier.astype(jnp.int32), axis=1)
    offsets = jax.random.randint(fourth, (count,), 0, SLOTS_DEV)
    slot = ((offsets[owner] + rank) % SLOTS_DEV).astype(jnp.int32)
    return (owner, slot)


def draw_page_owner(key, part):
    return page_table(key)[0]


def draw_page_slot(key, part):
    return page_table(key)[1]


def set_ends(result, key, low, high):
    place = [jax.random.randint(jax.random.fold_in(key, axis), (), 0, length) for axis, length in enumerate(result.shape)]
    main_axis = result.shape.index(max(result.shape))
    next_to = place[:main_axis] + [(place[main_axis] + 1) % result.shape[main_axis]] + place[main_axis + 1:]
    return result.at[tuple(place)].set(low).at[tuple(next_to)].set(high)


def block_scale(rng, dims, pieces, least, high):
    level = 1.0
    for dim, parts in pieces:
        draws = jax.random.uniform(jax.random.fold_in(jax.random.fold_in(rng, 6), dim), (parts,), jnp.float32, least / len(pieces), high / len(pieces))
        level = level * jnp.repeat(jnp.exp(draws), dims[dim] // parts).reshape((-1,) + (1,) * (len(dims) - 1 - dim))
    return level


def profile(amount, total, reach, slope):
    weights = [(1 << 20) // math.isqrt(rank ** slope) + 1 for rank in range(2, amount + 1)]
    surplus, given = total - reach - (amount - 1), [1] * (amount - 1)
    while surplus > 0:
        movable = [i for i in range(amount - 1) if given[i] < reach]
        pool, left = sum([weights[i] for i in movable]), surplus
        for i in movable:
            addition = min(reach - given[i], max(1, left * weights[i] // pool), surplus)
            given[i] = given[i] + addition
            surplus = surplus - addition
    return np.array([reach] + given)


def uneven_parts(stream_key, amount, total, most, lean):
    if amount == 2:
        one = jax.random.randint(stream_key, (), max(1, total - most), min(most, total - 1) + 1)
        return jnp.stack([one, total - one])
    sizes = jnp.asarray(profile(amount, total, most, lean), jnp.int32)
    couples = (amount - 1) // 2
    giver, receiver = sizes[1:1 + 2 * couples:2], sizes[2:2 + 2 * couples:2]
    room = jnp.minimum(giver - 1, most - receiver)
    shifted = jax.random.randint(jax.random.fold_in(stream_key, 1), (couples,), 0, 1 << 20) % (room + 1)
    sizes = sizes.at[1:1 + 2 * couples:2].set(giver - shifted).at[2:2 + 2 * couples:2].set(receiver + shifted)
    return sizes[jax.random.permutation(jax.random.fold_in(stream_key, 2), amount)]


def noise(own_key, dims, spread, most, pieces=(), held_as=jnp.bfloat16):
    values = spread * jax.random.normal(own_key, dims, jnp.float32)
    if pieces:
        values = values * block_scale(own_key, dims, pieces, -0.22, 0.18)
    return jnp.clip(values, -most, most).astype(held_as)


def setup_inputs(seed: int = 0) -> dict:
    seeds = jax.random.split(jax.random.key(seed), 14)
    return {
        "hidden": noise(seeds[0], (TOKENS, D), 1.0, 6.0, ((0, 16), (1, 2))),
        "key_weight": noise(seeds[1], (D, KVH * HD), D ** -0.5, 0.0625, ((0, 2),)),
        "value_weight": noise(seeds[2], (D, KVH * HD), D ** -0.5, 0.0625, ((0, 2),)),
        "key_bias": noise(seeds[3], (KVH * HD,), 1.0, 5.0, ((0, 2),), jnp.float32),
        "value_bias": noise(seeds[4], (KVH * HD,), 1.0, 5.0, ((0, 2),), jnp.float32),
        "request_tokens": uneven_parts(seeds[5], REQS, TOKENS, TOKENS // 8, 2).astype(jnp.int32),
        "request_context": set_ends(jax.random.randint(seeds[6], (REQS,), 0, 4096), jax.random.fold_in(seeds[6], 1), 0, 4095).astype(jnp.int32),
        "page_owner": draw_page_owner(jax.random.fold_in(seeds[13], 71), 0),
        "page_slot": draw_page_slot(jax.random.fold_in(seeds[13], 71), 0),
        "key_cache": jnp.clip(jax.random.uniform(seeds[9], (SLOTS, PAGE, KVH * HD), jnp.float32, -1.0, 1.0) * block_scale(seeds[9], (SLOTS, PAGE, KVH * HD), ((0, 16), (2, 2)), -0.4, 0.0), -1.0, 1.0).astype(jnp.bfloat16),
        "value_cache": jnp.clip(jax.random.uniform(seeds[10], (SLOTS, PAGE, KVH * HD), jnp.float32, -1.0, 1.0) * block_scale(seeds[10], (SLOTS, PAGE, KVH * HD), ((0, 16), (2, 2)), -0.4, 0.0), -1.0, 1.0).astype(jnp.bfloat16),
        "stored_key_scales": jnp.clip(jnp.exp(math.log(8.0) - 2.7725887 * jax.random.uniform(seeds[11], (SLOTS, KVH), jnp.float32) ** block_scale(seeds[11], (SLOTS, KVH), ((0, 16), (1, 2)), -0.2, 0.2)), 0.5, 8.0).astype(jnp.bfloat16),
        "value_scales": jnp.clip(jnp.exp(math.log(8.0) - 2.7725887 * jax.random.uniform(seeds[12], (SLOTS, KVH), jnp.float32) ** block_scale(seeds[12], (SLOTS, KVH), ((0, 16), (1, 2)), -0.2, 0.2)), 0.5, 8.0).astype(jnp.bfloat16),
    }


rope_base = 1000000.0
eps = 1e-6


def positions_of(request_tokens, request_context, token_ids):
    ends = jnp.cumsum(request_tokens).astype(jnp.int32)
    starts = ends - request_tokens
    inside = (token_ids[:, None] >= starts[None, :]) & (token_ids[:, None] < ends[None, :])
    offset = jnp.sum(jnp.where(inside, (request_context - starts)[None, :], 0), axis=1).astype(jnp.int32)
    return offset + token_ids


def rotate(values, positions, head_dim):
    half = head_dim // 2
    freqs = jnp.exp(-jnp.log(jnp.float32(rope_base)) * (2.0 * jnp.arange(half).astype(jnp.float32) / head_dim))
    angle = positions.astype(jnp.float32)[:, None] * freqs[None, :]
    cosine = jnp.cos(angle)[:, None, :]
    sine = jnp.sin(angle)[:, None, :]
    first = values[..., :half]
    second = values[..., half:]
    return jnp.concatenate([first * cosine - second * sine, second * cosine + first * sine], axis=-1)


def normalize(pages):
    largest = jnp.max(jnp.abs(pages.astype(jnp.float32)), axis=(1, 3))
    scale = (largest + eps).astype(jnp.bfloat16)
    codes = (pages.astype(jnp.float32) / scale.astype(jnp.float32)[:, None, :, None]).astype(jnp.bfloat16)
    return codes, scale


def reference(hidden, key_weight, value_weight, key_bias, value_bias, request_tokens, request_context, page_owner, page_slot, key_cache, value_cache, stored_key_scales, value_scales):
    token_ids = jnp.arange(TOKENS).astype(jnp.int32)
    positions = positions_of(request_tokens, request_context, token_ids)
    key_raw = jnp.dot(hidden, key_weight, preferred_element_type=jnp.float32) + key_bias
    value_raw = jnp.dot(hidden, value_weight, preferred_element_type=jnp.float32) + value_bias
    keys = rotate(key_raw.reshape(TOKENS, KVH, HD), positions, HD).astype(jnp.bfloat16)
    values = value_raw.reshape(TOKENS, KVH, HD).astype(jnp.bfloat16)
    key_codes, key_page_scale = normalize(keys.reshape(PAGES, PAGE, KVH, HD))
    value_codes, value_scale = normalize(values.reshape(PAGES, PAGE, KVH, HD))
    target = (page_owner * SLOTS_DEV + page_slot).astype(jnp.int32)
    new_key_cache = key_cache.at[target].set(key_codes.reshape(PAGES, PAGE, KVH * HD))
    new_value_cache = value_cache.at[target].set(value_codes.reshape(PAGES, PAGE, KVH * HD))
    new_key_scales = stored_key_scales.at[target].set(key_page_scale)
    new_value_scales = value_scales.at[target].set(value_scale)
    return new_key_cache, new_value_cache, new_key_scales, new_value_scales
```

```python
import functools

import jax
import jax.numpy as jnp
from jax import lax
from jax.experimental import pallas as pl
from jax.experimental.pallas import tpu as pltpu
from jax.sharding import PartitionSpec as P

rope_base = 1000000.0
eps = 1e-06
KS = 4
MESH = pl.DeviceIdType.MESH


def body(
    n, cap, heads, hd, page,
    dk_ref, sr_ref, cos_ref, sin_ref, kb_ref, vb_ref, oks_ref, ovs_ref,
    h_hbm, kw_hbm, vw_hbm, kc_hbm, vc_hbm,
    kc_out, vc_out, ks_out, vs_out,
    h_v, w_v, p_v, u_v, part_s, part_r, own_v, bias_v, send_v, recv_v, cache_v, scale_v,
    h_sem, w_sem, c_sem, o_sem, ps_sem, pr_sem, s_sem, r_sem, l_sem,
):
    toks, kd = h_v.shape[1:]
    depth = KS * kd
    wide = 2 * hd
    half_cols = heads * hd
    per = half_cols // wide
    chunks = 2 * per

    me = lax.axis_index("seq")
    side = lax.axis_index("head")
    other = 1 - side
    slots = cache_v.shape[1]

    def w_copy(c, o, s):
        src = vw_hbm if c < per else kw_hbm
        col = (other if o == 0 else side) * half_cols + (c % per) * wide
        col = pl.multiple_of(col, wide)
        return pltpu.make_async_copy(
            src.at[pl.ds(s * kd, kd), pl.ds(col, wide)],
            w_v.at[c, o, pl.ds(s * kd, kd)],
            w_sem.at[c, o, s],
        )

    def h_copy(s):
        return pltpu.make_async_copy(
            h_hbm.at[:, pl.ds(s * kd, kd)], h_v.at[s], h_sem.at[s]
        )

    def cache_in(c):
        src = vc_hbm if c < per else kc_hbm
        return pltpu.make_async_copy(
            src.at[:, :, pl.ds((c % per) * wide, wide)], cache_v.at[c], c_sem.at[c]
        )

    def cache_out(c):
        dst = vc_out if c < per else kc_out
        return pltpu.make_async_copy(
            cache_v.at[c], dst.at[:, :, pl.ds((c % per) * wide, wide)], o_sem.at[c]
        )

    for s in range(KS):
        h_copy(s).start()
        w_copy(0, 0, s).start()
    for c in range(chunks):
        for o in range(2):
            if (c, o) != (0, 0):
                for s in range(KS):
                    w_copy(c, o, s).start()
    for c in range(chunks):
        cache_in(c).start()

    barrier = pltpu.get_barrier_semaphore()
    pl.semaphore_signal(barrier, inc=1, device_id={"head": other}, device_id_type=MESH)

    def greet(k, carry):
        pl.semaphore_signal(
            barrier, inc=1, device_id={"seq": lax.rem(me + k, n)}, device_id_type=MESH
        )
        return carry

    lax.fori_loop(1, n, greet, 0)

    for c in range(chunks):
        src = vb_ref if c < per else kb_ref
        bias_v[c] = src[:, pl.ds((c % per) * wide, wide)]
    rows = lax.broadcasted_iota(jnp.int32, p_v.shape, 0)
    p_v[...] = (rows == dk_ref[...]).astype(jnp.float32).astype(jnp.bfloat16)
    lanes = lax.broadcasted_iota(jnp.int32, u_v.shape, 1)
    u_v[...] = (lanes == sr_ref[...]).astype(jnp.float32).astype(jnp.bfloat16)
    scale_v[...] = jnp.zeros_like(scale_v)

    def partial(c, o, out, first):
        def step(s, carry):
            @pl.when(jnp.logical_and(c == 0, first))
            def _():
                pltpu.make_async_copy(h_v.at[s], h_v.at[s], h_sem.at[s]).wait()

            w_slice = w_v.at[c, o, pl.ds(pl.multiple_of(s * kd, kd), kd)]
            pltpu.make_async_copy(w_slice, w_slice, w_sem.at[c, o, s]).wait()
            got = jnp.dot(h_v[s], w_slice[...], preferred_element_type=jnp.float32)

            @pl.when(s == 0)
            def _():
                out[...] = got

            @pl.when(s > 0)
            def _():
                out[...] = out[...] + got

            return carry

        lax.fori_loop(0, KS, step, 0)

    def produce(c, carry):
        partial(c, 0, part_s.at[c], True)

        @pl.when(c == 0)
        def _():
            pl.semaphore_wait(barrier, n)

        swap = pltpu.make_async_remote_copy(
            src_ref=part_s.at[c],
            dst_ref=part_r.at[c],
            send_sem=ps_sem.at[c],
            recv_sem=pr_sem.at[c],
            device_id={"head": other},
            device_id_type=MESH,
        )
        swap.start()
        partial(c, 1, own_v, False)
        swap.wait()
        total = own_v[...] + part_r[c] + bias_v[c]
        is_key = c >= per
        cosine = jnp.where(is_key, cos_ref[...], 1.0)
        sine = jnp.where(is_key, sin_ref[...], 0.0)
        pieces = []
        for j in range(2):
            x = total[:, j * hd:(j + 1) * hd]
            pieces.append(x * cosine + pltpu.roll(x, hd // 2, 1) * sine)
        rounded = jnp.concatenate(pieces, axis=1).astype(jnp.bfloat16)
        placed = jnp.dot(p_v[...], rounded, preferred_element_type=jnp.float32)
        left = placed[:, :hd].reshape(n * cap, page, hd)
        right = placed[:, hd:].reshape(n * cap, page, hd)
        send_v[c] = jnp.concatenate([left, right], axis=1).astype(jnp.bfloat16)
        pltpu.make_async_copy(
            send_v.at[c, pl.ds(0, cap)], recv_v.at[c, pl.ds(0, cap)], l_sem.at[c]
        ).start()

        def send(j, carry2):
            k = n // 2 + (1 - 2 * (j % 2)) * ((j + 1) // 2)
            pltpu.make_async_remote_copy(
                src_ref=send_v.at[c, pl.ds(k * cap, cap)],
                dst_ref=recv_v.at[c, pl.ds(k * cap, cap)],
                send_sem=s_sem.at[c],
                recv_sem=r_sem.at[c],
                device_id={"seq": lax.rem(me + k, n)},
                device_id_type=MESH,
            ).start()
            return carry2

        lax.fori_loop(0, n - 1, send, 0)
        return carry

    lax.fori_loop(0, chunks, produce, 0)

    head_lane = lax.broadcasted_iota(jnp.int32, (1, 1, hd), 2)
    sr = sr_ref[...]
    written = (sr >= 0)[: slots * page]

    def consume(c, carry):
        pltpu.make_async_copy(
            recv_v.at[c, pl.ds(0, cap)], recv_v.at[c, pl.ds(0, cap)], l_sem.at[c]
        ).wait()
        rest = recv_v.at[c, pl.ds(cap, (n - 1) * cap)]
        pltpu.make_async_copy(rest, rest, r_sem.at[c]).wait()
        pltpu.make_async_copy(cache_v.at[c], cache_v.at[c], c_sem.at[c]).wait()
        got = recv_v[c].astype(jnp.float32)
        coded = []
        for j in range(2):
            x = got[:, j * page:(j + 1) * page, :]
            largest = jnp.max(jnp.max(jnp.abs(x), axis=1, keepdims=True), axis=2, keepdims=True)
            scale = (largest + eps).astype(jnp.bfloat16).astype(jnp.float32)
            scale_v[...] += jnp.where(head_lane == 2 * c + j, scale, 0.0)
            coded.append((x / scale).reshape(n * cap * page, hd))
        codes = jnp.concatenate(coded, axis=1).astype(jnp.bfloat16)
        placed = jnp.dot(u_v[...], codes, preferred_element_type=jnp.float32)
        placed = placed[: slots * page]
        old = cache_v[c].astype(jnp.float32).reshape(slots * page, wide)
        cache_v[c] = (
            jnp.where(written, placed, old).reshape(slots, page, wide).astype(jnp.bfloat16)
        )
        for i in range(chunks):
            @pl.when(c == i)
            def _():
                cache_out(i).start()
        return carry

    lax.fori_loop(0, chunks, consume, 0)

    flat = jnp.broadcast_to(scale_v[...], (n * cap, page, hd)).reshape(n * cap * page, hd)
    spread = jnp.dot(u_v[...], flat.astype(jnp.bfloat16), preferred_element_type=jnp.float32)
    spread = spread[: slots * page].reshape(slots, page, hd)[:, 0, :]
    hit = jnp.max(
        jnp.where(written, 1.0, 0.0).reshape(slots, page, 1), axis=1
    ) > 0.5
    vs_out[...] = jnp.where(
        hit, spread[:, :heads], ovs_ref[...].astype(jnp.float32)
    ).astype(jnp.bfloat16)
    ks_out[...] = jnp.where(
        hit, spread[:, heads:2 * heads], oks_ref[...].astype(jnp.float32)
    ).astype(jnp.bfloat16)

    for c in range(chunks):
        cache_out(c).wait()
        out = send_v.at[c, pl.ds(cap, (n - 1) * cap)]
        pltpu.make_async_copy(out, out, s_sem.at[c]).wait()


def shards(
    hidden,
    key_weight,
    value_weight,
    key_bias,
    value_bias,
    request_tokens,
    request_context,
    page_owner,
    page_slot,
    key_cache,
    value_cache,
    stored_key_scales,
    value_scales,
):
    toks, depth = hidden.shape
    slots, page, cols = key_cache.shape
    heads = stored_key_scales.shape[1]
    hd = cols // heads
    pages_here = toks // page
    n = lax.axis_size("seq")
    me = lax.axis_index("seq")
    cap = (pages_here + n - 1) // n + 1
    half = hd // 2
    rows = n * cap * page
    srows = (slots * page + 15) // 16 * 16

    ends = jnp.cumsum(request_tokens)
    starts = ends - request_tokens
    token_ids = me * toks + jnp.arange(toks)
    inside = (token_ids[:, None] >= starts[None, :]) & (token_ids[:, None] < ends[None, :])
    offset = jnp.sum(jnp.where(inside, (request_context - starts)[None, :], 0), axis=1)
    positions = (offset + token_ids).astype(jnp.float32)
    freqs = jnp.exp(
        -jnp.log(jnp.float32(rope_base)) * (2.0 * jnp.arange(half).astype(jnp.float32) / hd)
    )
    angle = positions[:, None] * freqs[None, :]
    cosine, sine = jnp.cos(angle), jnp.sin(angle)
    cos_t = jnp.concatenate([cosine, cosine], axis=1)
    sin_t = jnp.concatenate([-sine, sine], axis=1)

    owners = page_owner.reshape(n, pages_here)
    within = jnp.arange(pages_here)
    before = (owners[:, :, None] == owners[:, None, :]) & (
        within[None, None, :] < within[None, :, None]
    )
    rank = jnp.sum(before.astype(jnp.int32), axis=2)
    own_owner = lax.dynamic_index_in_dim(owners, me, 0, keepdims=False)
    own_rank = lax.dynamic_index_in_dim(rank, me, 0, keepdims=False)
    place = lax.rem(own_owner - me + n, n) * cap + own_rank
    dk = (place[:, None] * page + jnp.arange(page)[None, :]).reshape(1, toks)
    senders = jnp.arange(n)
    lane = lax.rem(me - senders + n, n)[:, None] * cap + rank
    mine = owners == me
    hit = (page_slot.reshape(1, -1) == jnp.arange(srows // page)[:, None]) & mine.reshape(1, -1)
    src = jnp.sum(jnp.where(hit, lane.reshape(1, -1) + 1, 0), axis=1) - 1
    sr = jnp.where(
        src[:, None] >= 0, src[:, None] * page + jnp.arange(page)[None, :], -1
    ).reshape(srows, 1)

    wide = 2 * hd
    chunks = 2 * (cols // wide)
    vm = pl.BlockSpec(memory_space=pltpu.VMEM)
    hbm = pl.BlockSpec(memory_space=pl.ANY)
    f32, b16 = jnp.float32, jnp.bfloat16
    return pl.pallas_call(
        functools.partial(body, n, cap, heads, hd, page),
        out_shape=(
            jax.ShapeDtypeStruct(key_cache.shape, b16),
            jax.ShapeDtypeStruct(value_cache.shape, b16),
            jax.ShapeDtypeStruct(stored_key_scales.shape, b16),
            jax.ShapeDtypeStruct(value_scales.shape, b16),
        ),
        in_specs=[vm] * 8 + [hbm] * 5,
        out_specs=(hbm, hbm, vm, vm),
        scratch_shapes=[
            pltpu.VMEM((KS, toks, depth // KS), b16),
            pltpu.VMEM((chunks, 2, depth, wide), b16),
            pltpu.VMEM((rows, toks), b16),
            pltpu.VMEM((srows, rows), b16),
            pltpu.VMEM((chunks, toks, wide), f32),
            pltpu.VMEM((chunks, toks, wide), f32),
            pltpu.VMEM((toks, wide), f32),
            pltpu.VMEM((chunks, 1, wide), f32),
            pltpu.VMEM((chunks, n * cap, 2 * page, hd), b16),
            pltpu.VMEM((chunks, n * cap, 2 * page, hd), b16),
            pltpu.VMEM((chunks, slots, page, wide), b16),
            pltpu.VMEM((n * cap, 1, hd), f32),
            pltpu.SemaphoreType.DMA((KS,)),
            pltpu.SemaphoreType.DMA((chunks, 2, KS)),
            pltpu.SemaphoreType.DMA((chunks,)),
            pltpu.SemaphoreType.DMA((chunks,)),
            pltpu.SemaphoreType.DMA((chunks,)),
            pltpu.SemaphoreType.DMA((chunks,)),
            pltpu.SemaphoreType.DMA((chunks,)),
            pltpu.SemaphoreType.DMA((chunks,)),
            pltpu.SemaphoreType.DMA((chunks,)),
        ],
        compiler_params=pltpu.CompilerParams(
            collective_id=0, has_side_effects=True, vmem_limit_bytes=60 * 1024 * 1024
        ),
    )(
        dk, sr, cos_t, sin_t, key_bias.reshape(1, -1), value_bias.reshape(1, -1),
        stored_key_scales, value_scales, hidden, key_weight, value_weight,
        key_cache, value_cache,
    )


def solution(mesh):
    placed = (
        P("seq", "head"),
        P("head", None),
        P("head", None),
        P("head"),
        P("head"),
        P(),
        P(),
        P(),
        P(),
        P("seq", None, "head"),
        P("seq", None, "head"),
        P("seq", "head"),
        P("seq", "head"),
    )
    return jax.shard_map(
        shards,
        mesh=mesh,
        in_specs=placed,
        out_specs=(
            P("seq", None, "head"),
            P("seq", None, "head"),
            P("seq", "head"),
            P("seq", "head"),
        ),
        check_vma=False,
    )
```

```python
import functools

import jax
import jax.numpy as jnp
from jax import lax
from jax.experimental import pallas as pl
from jax.experimental.pallas import tpu as pltpu
from jax.sharding import PartitionSpec as P

rope_base = 1000000.0
eps = 1e-06
KS = 4
MESH = pl.DeviceIdType.MESH


def body(
    n, cap, heads, hd, page,
    own_in, slot_in, freq_in, kb_in, vb_in, oks_in, ovs_in, rt_in, rc_in,
    h_hbm, kw_hbm, vw_hbm, kc_hbm, vc_hbm,
    kc_out, vc_out, ks_out, vs_out,
    h_v, w_v, p_v, u_v, part_s, part_r, own_v, bias_v, send_v, recv_v, cache_v, scale_v,
    cos_v, sin_v, sr_v,
    own_ref, slot_ref, freq_ref, kb_ref, vb_ref, oks_ref, ovs_ref, rt_ref, rc_ref,
    h_sem, w_sem, c_sem, o_sem, ps_sem, pr_sem, s_sem, r_sem, l_sem, i_sem,
):
    toks, kd = h_v.shape[1:]
    depth = KS * kd
    wide = 2 * hd
    half_cols = heads * hd
    per = half_cols // wide
    chunks = 2 * per

    me = lax.axis_index("seq")
    side = lax.axis_index("head")
    other = 1 - side
    slots = cache_v.shape[1]

    def w_copy(c, o, s):
        src = vw_hbm if c < per else kw_hbm
        col = (other if o == 0 else side) * half_cols + (c % per) * wide
        col = pl.multiple_of(col, wide)
        return pltpu.make_async_copy(
            src.at[pl.ds(s * kd, kd), pl.ds(col, wide)],
            w_v.at[c, o, pl.ds(s * kd, kd)],
            w_sem.at[c, o, s],
        )

    def h_copy(s):
        return pltpu.make_async_copy(
            h_hbm.at[:, pl.ds(s * kd, kd)], h_v.at[s], h_sem.at[s]
        )

    def cache_in(c):
        src = vc_hbm if c < per else kc_hbm
        return pltpu.make_async_copy(
            src.at[:, :, pl.ds((c % per) * wide, wide)], cache_v.at[c], c_sem.at[c]
        )

    def cache_out(c):
        dst = vc_out if c < per else kc_out
        return pltpu.make_async_copy(
            cache_v.at[c], dst.at[:, :, pl.ds((c % per) * wide, wide)], o_sem.at[c]
        )

    pairs = (
        (own_in, own_ref), (slot_in, slot_ref), (freq_in, freq_ref), (kb_in, kb_ref),
        (vb_in, vb_ref), (oks_in, oks_ref), (ovs_in, ovs_ref), (rt_in, rt_ref), (rc_in, rc_ref),
    )
    small = [
        pltpu.make_async_copy(src, dst, i_sem.at[i]) for i, (src, dst) in enumerate(pairs)
    ]
    for copy in small:
        copy.start()
    for s in range(KS):
        h_copy(s).start()
        w_copy(0, 0, s).start()
    for s in range(KS):
        w_copy(0, 1, s).start()

    barrier = pltpu.get_barrier_semaphore()
    pl.semaphore_signal(barrier, inc=1, device_id={"head": other}, device_id_type=MESH)

    def greet(k, carry):
        pl.semaphore_signal(
            barrier, inc=1, device_id={"seq": lax.rem(me + k, n)}, device_id_type=MESH
        )
        return carry

    lax.fori_loop(1, n, greet, 0)
    for copy in small:
        copy.wait()

    for c in range(chunks):
        src = vb_ref if c < per else kb_ref
        bias_v[c] = src[:, pl.ds((c % per) * wide, wide)]
    total_pages = own_ref.shape[1]
    here = total_pages // n
    f32 = jnp.float32
    owner = own_ref[...]
    gid = lax.broadcasted_iota(jnp.int32, (1, total_pages), 1)
    within = gid % here
    match = lax.broadcasted_iota(jnp.int32, (n, total_pages), 0) == owner
    count = jnp.where(match, 1.0, 0.0)
    shift = 1
    while shift < here:
        count = count + jnp.where(within >= shift, pltpu.roll(count, shift, 1), 0.0)
        shift *= 2
    rank = jnp.sum(jnp.where(match, count, 0.0), axis=0, keepdims=True) - 1.0
    place = ((owner - me + n) % n * cap).astype(f32) + rank
    place = pltpu.roll(
        jnp.broadcast_to(place, (8, total_pages)), (total_pages - me * here) % total_pages, 1
    )[:, :here]
    expand = (
        lax.broadcasted_iota(jnp.int32, (here, toks), 0)
        == lax.broadcasted_iota(jnp.int32, (here, toks), 1) // page
    )
    place = jnp.dot(
        place.astype(jnp.bfloat16),
        jnp.where(expand, 1.0, 0.0).astype(jnp.bfloat16),
        preferred_element_type=f32,
    )[:1]
    token = lax.broadcasted_iota(jnp.int32, (1, toks), 1)
    dk = place * page + (token % page).astype(f32)
    rows = lax.broadcasted_iota(jnp.int32, p_v.shape, 0).astype(f32)
    p_v[...] = jnp.where(rows == dk, 1.0, 0.0).astype(jnp.bfloat16)

    def unpack_table():
        slot = jnp.where(owner == me, slot_ref[...], -1)
        lane = (((me - gid // here + n) % n) * cap).astype(f32) + rank + 1.0
        want = lax.broadcasted_iota(jnp.int32, (u_v.shape[0], 1), 0)
        src = jnp.sum(jnp.where(want // page == slot, lane, 0.0), axis=1, keepdims=True) - 1.0
        sr_v[...] = jnp.where(src >= 0.0, src * page + (want % page).astype(f32), -1.0)
        lanes = lax.broadcasted_iota(jnp.int32, u_v.shape, 1).astype(f32)
        u_v[...] = jnp.where(lanes == sr_v[...], 1.0, 0.0).astype(jnp.bfloat16)

    def rope_table():
        token_ids = me * toks + lax.broadcasted_iota(jnp.int32, cos_v.shape, 0)
        offset = jnp.zeros_like(token_ids)
        start = jnp.int32(0)
        for r in range(rt_ref.shape[0]):
            offset = jnp.where(token_ids >= start, rc_ref[r] - start, offset)
            start = start + rt_ref[r]
        angle = (offset + token_ids).astype(f32) * freq_ref[...]
        cos_v[...] = jnp.cos(angle)
        sine = jnp.sin(angle)
        front = lax.broadcasted_iota(jnp.int32, cos_v.shape, 1) < hd // 2
        sin_v[...] = jnp.where(front, -sine, sine)

    cos_v[...] = jnp.ones_like(cos_v)
    sin_v[...] = jnp.zeros_like(sin_v)
    scale_v[...] = jnp.zeros_like(scale_v)

    def partial(c, o, out, first):
        def step(s, carry):
            @pl.when(jnp.logical_and(c == 0, first))
            def _():
                pltpu.make_async_copy(h_v.at[s], h_v.at[s], h_sem.at[s]).wait()

            w_slice = w_v.at[c, o, pl.ds(pl.multiple_of(s * kd, kd), kd)]
            pltpu.make_async_copy(w_slice, w_slice, w_sem.at[c, o, s]).wait()
            got = jnp.dot(h_v[s], w_slice[...], preferred_element_type=jnp.float32)

            @pl.when(s == 0)
            def _():
                out[...] = got

            @pl.when(s > 0)
            def _():
                out[...] = out[...] + got

            return carry

        lax.fori_loop(0, KS, step, 0)

    def produce(c, carry):
        for i in range(1, chunks):
            @pl.when(c == i - 1)
            def _():
                for o in range(2):
                    for s in range(KS):
                        w_copy(i, o, s).start()

        @pl.when(c == chunks - 2)
        def _():
            for i in range(chunks):
                cache_in(i).start()

        partial(c, 0, part_s.at[c], True)

        @pl.when(c == 0)
        def _():
            pl.semaphore_wait(barrier, n)

        swap = pltpu.make_async_remote_copy(
            src_ref=part_s.at[c],
            dst_ref=part_r.at[c],
            send_sem=ps_sem.at[c],
            recv_sem=pr_sem.at[c],
            device_id={"head": other},
            device_id_type=MESH,
        )
        swap.start()
        partial(c, 1, own_v, False)
        swap.wait()
        total = own_v[...] + part_r[c] + bias_v[c]
        cosine = cos_v[...]
        sine = sin_v[...]
        pieces = []
        for j in range(2):
            x = total[:, j * hd:(j + 1) * hd]
            pieces.append(x * cosine + pltpu.roll(x, hd // 2, 1) * sine)
        rounded = jnp.concatenate(pieces, axis=1).astype(jnp.bfloat16)
        placed = jnp.dot(p_v[...], rounded, preferred_element_type=jnp.float32)
        left = placed[:, :hd].reshape(n * cap, page, hd)
        right = placed[:, hd:].reshape(n * cap, page, hd)
        send_v[c] = jnp.concatenate([left, right], axis=1).astype(jnp.bfloat16)
        pltpu.make_async_copy(
            send_v.at[c, pl.ds(0, cap)], recv_v.at[c, pl.ds(0, cap)], l_sem.at[c]
        ).start()

        def send(j, carry2):
            k = n // 2 + (1 - 2 * (j % 2)) * ((j + 1) // 2)
            pltpu.make_async_remote_copy(
                src_ref=send_v.at[c, pl.ds(k * cap, cap)],
                dst_ref=recv_v.at[c, pl.ds(k * cap, cap)],
                send_sem=s_sem.at[c],
                recv_sem=r_sem.at[c],
                device_id={"seq": lax.rem(me + k, n)},
                device_id_type=MESH,
            ).start()
            return carry2

        lax.fori_loop(0, n - 1, send, 0)

        @pl.when(c == per - 1)
        def _():
            rope_table()

        return carry

    lax.fori_loop(0, chunks, produce, 0)

    unpack_table()
    head_lane = lax.broadcasted_iota(jnp.int32, (1, 1, hd), 2)
    written = (sr_v[...] >= 0.0)[: slots * page]

    def consume(c, carry):
        pltpu.make_async_copy(
            recv_v.at[c, pl.ds(0, cap)], recv_v.at[c, pl.ds(0, cap)], l_sem.at[c]
        ).wait()
        rest = recv_v.at[c, pl.ds(cap, (n - 1) * cap)]
        pltpu.make_async_copy(rest, rest, r_sem.at[c]).wait()
        pltpu.make_async_copy(cache_v.at[c], cache_v.at[c], c_sem.at[c]).wait()
        got = recv_v[c].astype(jnp.float32)
        coded = []
        for j in range(2):
            x = got[:, j * page:(j + 1) * page, :]
            largest = jnp.max(jnp.max(jnp.abs(x), axis=1, keepdims=True), axis=2, keepdims=True)
            scale = (largest + eps).astype(jnp.bfloat16).astype(jnp.float32)
            scale_v[...] += jnp.where(head_lane == 2 * c + j, scale, 0.0)
            coded.append((x / scale).reshape(n * cap * page, hd))
        codes = jnp.concatenate(coded, axis=1).astype(jnp.bfloat16)
        placed = jnp.dot(u_v[...], codes, preferred_element_type=jnp.float32)
        placed = placed[: slots * page]
        old = cache_v[c].astype(jnp.float32).reshape(slots * page, wide)
        cache_v[c] = (
            jnp.where(written, placed, old).reshape(slots, page, wide).astype(jnp.bfloat16)
        )
        for i in range(chunks):
            @pl.when(c == i)
            def _():
                cache_out(i).start()
        return carry

    lax.fori_loop(0, chunks, consume, 0)

    flat = jnp.broadcast_to(scale_v[...], (n * cap, page, hd)).reshape(n * cap * page, hd)
    spread = jnp.dot(u_v[...], flat.astype(jnp.bfloat16), preferred_element_type=jnp.float32)
    spread = spread[: slots * page].reshape(slots, page, hd)[:, 0, :]
    spread = jnp.concatenate([spread, jnp.zeros((128 - slots % 128, hd), f32)], axis=0)
    spread = jnp.transpose(spread)[:, :slots]
    vs_out[...] = jnp.where(
        spread[:heads] > 0.0, spread[:heads], ovs_ref[...].astype(f32)
    ).astype(jnp.bfloat16)
    ks_out[...] = jnp.where(
        spread[heads:2 * heads] > 0.0, spread[heads:2 * heads], oks_ref[...].astype(f32)
    ).astype(jnp.bfloat16)

    for c in range(chunks):
        cache_out(c).wait()
        out = send_v.at[c, pl.ds(cap, (n - 1) * cap)]
        pltpu.make_async_copy(out, out, s_sem.at[c]).wait()


def hand_on(pieces, *refs):
    srcs, dsts, held = refs[:4], refs[4:8], refs[8:12]
    in_sem, out_sem = refs[12:]
    views = []
    for src, dst, here in zip(srcs, dsts, held):
        if src.shape[0] >= 8:
            size = src.shape[0]
            cuts = [size * i // pieces for i in range(pieces + 1)]
            for low, high in zip(cuts, cuts[1:]):
                part = pl.ds(low, high - low)
                views.append((src.at[part], dst.at[part], here.at[part]))
        else:
            views.append((src, dst, here))
    ins = [pltpu.make_async_copy(v[0], v[2], in_sem.at[i]) for i, v in enumerate(views)]
    outs = [pltpu.make_async_copy(v[2], v[1], out_sem.at[i]) for i, v in enumerate(views)]
    for copy in ins:
        copy.start()
    for copy_in, copy_out in zip(ins, outs):
        copy_in.wait()
        copy_out.start()
    for copy in outs:
        copy.wait()


def shards(
    hidden,
    key_weight,
    value_weight,
    key_bias,
    value_bias,
    request_tokens,
    request_context,
    page_owner,
    page_slot,
    key_cache,
    value_cache,
    stored_key_scales,
    value_scales,
):
    toks, depth = hidden.shape
    slots, page, cols = key_cache.shape
    heads = stored_key_scales.shape[1]
    hd = cols // heads
    pages_here = toks // page
    n = lax.axis_size("seq")
    cap = (pages_here + n - 1) // n + 1
    half = hd // 2
    rows = n * cap * page
    srows = (slots * page + 15) // 16 * 16

    freqs = jnp.exp(
        -jnp.log(jnp.float32(rope_base)) * (2.0 * jnp.arange(half).astype(jnp.float32) / hd)
    )
    freqs = jnp.concatenate([freqs, freqs]).reshape(1, hd)
    wide = 2 * hd
    chunks = 2 * (cols // wide)
    vm = pl.BlockSpec(memory_space=pltpu.VMEM)
    hbm = pl.BlockSpec(memory_space=pl.ANY)
    f32, b16 = jnp.float32, jnp.bfloat16
    old_value_scales = value_scales
    done = pl.pallas_call(
        functools.partial(body, n, cap, heads, hd, page),
        out_shape=(
            jax.ShapeDtypeStruct(key_cache.shape, b16),
            jax.ShapeDtypeStruct(value_cache.shape, b16),
            jax.ShapeDtypeStruct((heads, slots), b16),
            jax.ShapeDtypeStruct((heads, slots), b16),
        ),
        in_specs=[hbm] * 14,
        out_specs=(hbm, hbm, vm, vm),
        scratch_shapes=[
            pltpu.VMEM((KS, toks, depth // KS), b16),
            pltpu.VMEM((chunks, 2, depth, wide), b16),
            pltpu.VMEM((rows, toks), b16),
            pltpu.VMEM((srows, rows), b16),
            pltpu.VMEM((chunks, toks, wide), f32),
            pltpu.VMEM((chunks, toks, wide), f32),
            pltpu.VMEM((toks, wide), f32),
            pltpu.VMEM((chunks, 1, wide), f32),
            pltpu.VMEM((chunks, n * cap, 2 * page, hd), b16),
            pltpu.VMEM((chunks, n * cap, 2 * page, hd), b16),
            pltpu.VMEM((chunks, slots, page, wide), b16),
            pltpu.VMEM((n * cap, 1, hd), f32),
            pltpu.VMEM((toks, hd), f32),
            pltpu.VMEM((toks, hd), f32),
            pltpu.VMEM((srows, 1), f32),
            pltpu.VMEM((1, page_owner.shape[0]), jnp.int32),
            pltpu.VMEM((1, page_owner.shape[0]), jnp.int32),
            pltpu.VMEM((1, hd), f32),
            pltpu.VMEM((1, cols), f32),
            pltpu.VMEM((1, cols), f32),
            pltpu.VMEM((heads, slots), b16),
            pltpu.VMEM((heads, slots), b16),
            pltpu.SMEM(request_tokens.shape, jnp.int32),
            pltpu.SMEM(request_tokens.shape, jnp.int32),
            pltpu.SemaphoreType.DMA((KS,)),
            pltpu.SemaphoreType.DMA((chunks, 2, KS)),
            pltpu.SemaphoreType.DMA((chunks,)),
            pltpu.SemaphoreType.DMA((chunks,)),
            pltpu.SemaphoreType.DMA((chunks,)),
            pltpu.SemaphoreType.DMA((chunks,)),
            pltpu.SemaphoreType.DMA((chunks,)),
            pltpu.SemaphoreType.DMA((chunks,)),
            pltpu.SemaphoreType.DMA((chunks,)),
            pltpu.SemaphoreType.DMA((9,)),
        ],
        compiler_params=pltpu.CompilerParams(
            collective_id=0, has_side_effects=True, vmem_limit_bytes=60 * 1024 * 1024
        ),
    )(
        page_owner.reshape(1, -1), page_slot.reshape(1, -1), freqs,
        key_bias.reshape(1, -1), value_bias.reshape(1, -1),
        stored_key_scales.T, old_value_scales.T, request_tokens, request_context,
        hidden, key_weight, value_weight, key_cache, value_cache,
    )
    pieces = 2
    moves = 2 * pieces + 2
    keys, values, key_scales, value_scales = pl.pallas_call(
        functools.partial(hand_on, pieces),
        out_shape=tuple(jax.ShapeDtypeStruct(a.shape, a.dtype) for a in done),
        in_specs=[hbm] * 4,
        out_specs=(hbm,) * 4,
        scratch_shapes=[pltpu.VMEM(a.shape, a.dtype) for a in done]
        + [pltpu.SemaphoreType.DMA((moves,)), pltpu.SemaphoreType.DMA((moves,))],
        compiler_params=pltpu.CompilerParams(vmem_limit_bytes=60 * 1024 * 1024),
    )(*done)
    return keys, values, key_scales.T, value_scales.T


def solution(mesh):
    placed = (
        P("seq", "head"),
        P("head", None),
        P("head", None),
        P("head"),
        P("head"),
        P(),
        P(),
        P(),
        P(),
        P("seq", None, "head"),
        P("seq", None, "head"),
        P("seq", "head"),
        P("seq", "head"),
    )
    return jax.shard_map(
        shards,
        mesh=mesh,
        in_specs=placed,
        out_specs=(
            P("seq", None, "head"),
            P("seq", None, "head"),
            P("seq", "head"),
            P("seq", "head"),
        ),
        check_vma=False,
    )
```
